32 devices in a mesh: rows: 16 (over z, x, core), cols: 2 (over y).
Axes of the slice: x: 2, y: 2, z: 4, core: 2. Of those that a mesh axis runs over, the one named last changes fastest.
Arguments:
- tokens: bfloat16 [32768, 1024], P('rows', 'cols'), may hold values from -6 to 6
- cotangent: bfloat16 [32768, 1024], P('rows', 'cols'), may hold values from -6 to 6
- first_gain: float32 [1024], replicated, may hold values from 0.5 to 1.5
- first_shift: float32 [1024], replicated, may hold values from -1.75 to 1.75
- second_gain: float32 [1024], replicated, may hold values from 0.5 to 1.5
- second_shift: float32 [1024], replicated, may hold values from -1.75 to 1.75
- query_weight: float32 [1024, 1024], P('rows', 'cols'), may hold values from -0.1875 to 0.1875
- key_weight: float32 [1024, 1024], P('rows', 'cols'), may hold values from -0.1875 to 0.1875
- value_weight: float32 [1024, 1024], P('rows', 'cols'), may hold values from -0.1875 to 0.1875
- query_bias: float32 [1024], P('cols'), may hold values from -3 to 3
- value_bias: float32 [1024], P('cols'), may hold values from -3 to 3
- output_weight: float32 [1024, 1024], P('cols', 'rows'), may hold values from -0.75 to 0.75
- up_weight: float32 [1024, 4096], P('rows', 'cols'), may hold values from -0.1875 to 0.1875
- up_bias: float32 [4096], P('cols'), may hold values from -3 to 3
- down_weight: float32 [4096, 1024], P('cols', 'rows'), may hold values from -0.09375 to 0.09375
- out_bias: float32 [1024], P('cols'), may hold values from -3 to 3
- first_gain_moment: float32 [1024], replicated, may hold values from -512 to 512
- first_shift_moment: float32 [1024], replicated, may hold values from -512 to 512
- second_gain_moment: float32 [1024], replicated, may hold values from -512 to 512
- second_shift_moment: float32 [1024], replicated, may hold values from -512 to 512
- query_moment: float32 [1024, 1024], P('rows', 'cols'), may hold values from -448 to 448
- key_moment: float32 [1024, 1024], P('rows', 'cols'), may hold values from -448 to 448
- value_moment: float32 [1024, 1024], P('rows', 'cols'), may hold values from -448 to 448
- query_bias_moment: float32 [1024], P('cols'), may hold values from -448 to 448
- value_bias_moment: float32 [1024], P('cols'), may hold values from -448 to 448
- output_moment: float32 [1024, 1024], P('cols', 'rows'), may hold values from -160 to 160
- up_moment: float32 [1024, 4096], P('rows', 'cols'), may hold values from -448 to 448
- up_bias_moment: float32 [4096], P('cols'), may hold values from -448 to 448
- down_moment: float32 [4096, 1024], P('cols', 'rows'), may hold values from -640 to 640
- out_bias_moment: float32 [1024], P('cols'), may hold values from -1024 to 1024
Outputs:
- result: bfloat16 [32768, 1024], P('rows', 'cols')
- tokens_grad: float32 [32768, 1024], P('rows', 'cols')
- first_gain_grad: float32 [1024], replicated
- first_shift_grad: float32 [1024], replicated
- second_gain_grad: float32 [1024], replicated
- second_shift_grad: float32 [1024], replicated
- query_weight_grad: float32 [1024, 1024], P('rows', 'cols')
- key_weight_grad: float32 [1024, 1024], P('rows', 'cols')
- value_weight_grad: float32 [1024, 1024], P('rows', 'cols')
- query_bias_grad: float32 [1024], P('cols')
- value_bias_grad: float32 [1024], P('cols')
- output_weight_grad: float32 [1024, 1024], P('cols', 'rows')
- up_weight_grad: float32 [1024, 4096], P('rows', 'cols')
- up_bias_grad: float32 [4096], P('cols')
- down_weight_grad: float32 [4096, 1024], P('cols', 'rows')
- out_bias_grad: float32 [1024], P('cols')
- first_gain_moment_new: float32 [1024], replicated
- first_shift_moment_new: float32 [1024], replicated
- second_gain_moment_new: float32 [1024], replicated
- second_shift_moment_new: float32 [1024], replicated
- query_moment_new: float32 [1024, 1024], P('rows', 'cols')
- key_moment_new: float32 [1024, 1024], P('rows', 'cols')
- value_moment_new: float32 [1024, 1024], P('rows', 'cols')
- query_bias_moment_new: float32 [1024], P('cols')
- value_bias_moment_new: float32 [1024], P('cols')
- output_moment_new: float32 [1024, 1024], P('cols', 'rows')
- up_moment_new: float32 [1024, 4096], P('rows', 'cols')
- up_bias_moment_new: float32 [4096], P('cols')
- down_moment_new: float32 [4096, 1024], P('cols', 'rows')
- out_bias_moment_new: float32 [1024], P('cols')
- first_gain_new: float32 [1024], replicated
- first_shift_new: float32 [1024], replicated
- second_gain_new: float32 [1024], replicated
- second_shift_new: float32 [1024], replicated
- query_weight_new: float32 [1024, 1024], P('rows', 'cols')
- key_weight_new: float32 [1024, 1024], P('rows', 'cols')
- value_weight_new: float32 [1024, 1024], P('rows', 'cols')
- query_bias_new: float32 [1024], P('cols')
- value_bias_new: float32 [1024], P('cols')
- output_weight_new: float32 [1024, 1024], P('cols', 'rows')
- up_weight_new: float32 [1024, 4096], P('rows', 'cols')
- up_bias_new: float32 [4096], P('cols')
- down_weight_new: float32 [4096, 1024], P('cols', 'rows')
- out_bias_new: float32 [1024], P('cols')
The draws below stay inside these ranges and needn't reach their ends.
All inputs are finite; a program needn't handle non-finite values.
Results may differ from the reference program's by a relative error of at most 0.012.
The reference program's roundings to bfloat16 on the way count: a program that leaves them out, or rounds other values in their place, can miss the bound.
Values may be sent and summed in bfloat16 or wider, within the bound.
A program may use at most 256 MiB of HBM per device.

```python
import math
from functools import partial
import jax
import jax.numpy as jnp
from jax import lax

D = 1024
HD = 64
ROT = 16
FF = 4096
LEN = 1024
BLOCK = 512
ITERS = 5
TOK_DEV = 2048
TOKENS = 32768


def raised(drawn, own_key, source, target, parts, factor):
    owner, partner = [(jnp.arange(drawn.shape[dim]) // (drawn.shape[dim] // parts)).reshape([-1 if axis == dim else 1 for axis in range(drawn.ndim)]) for dim in (source, target)]
    chosen = jax.random.permutation(own_key, parts)[partner]
    strong = (owner == chosen) | (owner == (partner + parts // 2) % parts)
    return jnp.where(strong, factor * drawn, drawn)


def steps_of(rng, shape, pieces, smallest, high):
    gain = 1.0
    for dim, blocks in pieces:
        draws = jax.random.uniform(jax.random.fold_in(jax.random.fold_in(rng, 6), dim), (blocks,), jnp.float32, smallest / len(pieces), high / len(pieces))
        gain = gain * jnp.repeat(jnp.exp(draws), shape[dim] // blocks).reshape((-1,) + (1,) * (len(shape) - 1 - dim))
    return gain


def scatter_about(rng, extent, scale, bound, cuts=(), held_as=jnp.bfloat16):
    drawn = scale * jax.random.normal(rng, extent, jnp.float32)
    if cuts:
        drawn = drawn * steps_of(rng, extent, cuts, -0.22, 0.18)
    return jnp.clip(drawn, -bound, bound).astype(held_as)


def noise_with(rng, extent, deviation, reach, pieces, heavy, kind=jnp.bfloat16):
    entries = deviation * jax.random.normal(rng, extent, jnp.float32)
    if pieces:
        entries = entries * steps_of(rng, extent, pieces, -0.22, 0.18)
    return jnp.clip(raised(entries, jax.random.fold_in(rng, 3), *heavy), -reach, reach).astype(kind)


def setup_inputs(seed: int = 0) -> dict:
    streams_of = jax.random.split(jax.random.key(seed), 31)
    tokens = noise_with(streams_of[0], (TOKENS, D), 1.0, 6.0, ((0, 16), (1, 2)), (0, 1, 16, 2.0))
    cotangent = noise_with(streams_of[1], (TOKENS, D), 1.0, 6.0, ((0, 16), (1, 2)), (0, 1, 16, 2.0))
    first_gain = jnp.clip(1.0 + 0.1 * jax.random.normal(streams_of[2], (D,), jnp.float32), 0.5, 1.5)
    first_shift = scatter_about(streams_of[3], (D,), 0.3, 1.75, (), jnp.float32)
    second_gain = jnp.clip(1.0 + 0.1 * jax.random.normal(streams_of[4], (D,), jnp.float32), 0.5, 1.5)
    second_shift = scatter_about(streams_of[5], (D,), 0.3, 1.75, (), jnp.float32)
    query_weight = scatter_about(streams_of[6], (D, D), D ** -0.5, 0.1875, ((0, 16), (1, 2)), jnp.float32)
    key_weight = scatter_about(streams_of[7], (D, D), D ** -0.5, 0.1875, ((0, 16), (1, 2)), jnp.float32)
    value_weight = scatter_about(streams_of[8], (D, D), D ** -0.5, 0.1875, ((0, 16), (1, 2)), jnp.float32)
    query_bias = scatter_about(streams_of[9], (D,), 0.5, 3.0, ((0, 2),), jnp.float32)
    value_bias = scatter_about(streams_of[10], (D,), 0.5, 3.0, ((0, 2),), jnp.float32)
    output_weight = scatter_about(streams_of[11], (D, D), (D // 16) ** -0.5, 0.75, ((0, 2), (1, 16)), jnp.float32)
    up_weight = scatter_about(streams_of[12], (D, FF), D ** -0.5, 0.1875, ((0, 16), (1, 2)), jnp.float32)
    up_bias = scatter_about(streams_of[13], (FF,), 0.5, 3.0, ((0, 2),), jnp.float32)
    down_weight = scatter_about(streams_of[14], (FF, D), FF ** -0.5, 0.09375, ((0, 2), (1, 16)), jnp.float32)
    out_bias = scatter_about(streams_of[15], (D,), 0.5, 3.0, ((0, 2),), jnp.float32)
    first_gain_moment = scatter_about(streams_of[16], (D,), (TOKENS ** 0.5 * 0.5), 512.0, (), jnp.float32)
    first_shift_moment = scatter_about(streams_of[17], (D,), (TOKENS ** 0.5 * 0.5), 512.0, (), jnp.float32)
    second_gain_moment = scatter_about(streams_of[18], (D,), (TOKENS ** 0.5 * 0.5), 512.0, (), jnp.float32)
    second_shift_moment = scatter_about(streams_of[19], (D,), (TOKENS ** 0.5 * 0.5), 512.0, (), jnp.float32)
    query_moment = scatter_about(streams_of[20], (D, D), (TOKENS ** 0.5 * 0.4), 448.0, ((0, 16), (1, 2)), jnp.float32)
    key_moment = scatter_about(streams_of[21], (D, D), (TOKENS ** 0.5 * 0.4), 448.0, ((0, 16), (1, 2)), jnp.float32)
    value_moment = scatter_about(streams_of[22], (D, D), (TOKENS ** 0.5 * 0.4), 448.0, ((0, 16), (1, 2)), jnp.float32)
    query_bias_moment = scatter_about(streams_of[23], (D,), (TOKENS ** 0.5 * 0.4), 448.0, ((0, 2),), jnp.float32)
    value_bias_moment = scatter_about(streams_of[24], (D,), (TOKENS ** 0.5 * 0.4), 448.0, ((0, 2),), jnp.float32)
    output_moment = scatter_about(streams_of[25], (D, D), (TOKENS ** 0.5 * 0.15), 160.0, ((0, 2), (1, 16)), jnp.float32)
    up_moment = scatter_about(streams_of[26], (D, FF), (TOKENS ** 0.5 * 0.4), 448.0, ((0, 16), (1, 2)), jnp.float32)
    up_bias_moment = scatter_about(streams_of[27], (FF,), (TOKENS ** 0.5 * 0.4), 448.0, ((0, 2),), jnp.float32)
    down_moment = scatter_about(streams_of[28], (FF, D), (TOKENS ** 0.5 * 0.6), 640.0, ((0, 2), (1, 16)), jnp.float32)
    out_bias_moment = scatter_about(streams_of[29], (D,), (TOKENS ** 0.5 * 1.0), 1024.0, ((0, 2),), jnp.float32)
    return dict(tokens=tokens, cotangent=cotangent, first_gain=first_gain, first_shift=first_shift, second_gain=second_gain, second_shift=second_shift, query_weight=query_weight, key_weight=key_weight, value_weight=value_weight, query_bias=query_bias, value_bias=value_bias, output_weight=output_weight, up_weight=up_weight, up_bias=up_bias, down_weight=down_weight, out_bias=out_bias, first_gain_moment=first_gain_moment, first_shift_moment=first_shift_moment, second_gain_moment=second_gain_moment, second_shift_moment=second_shift_moment, query_moment=query_moment, key_moment=key_moment, value_moment=value_moment, query_bias_moment=query_bias_moment, value_bias_moment=value_bias_moment, output_moment=output_moment, up_moment=up_moment, up_bias_moment=up_bias_moment, down_moment=down_moment, out_bias_moment=out_bias_moment)


@jax.custom_vjp
def low(v):
    return lax.optimization_barrier(v.astype(jnp.bfloat16)).astype(jnp.float32)

@jax.custom_vjp
def low_back(v):
    return v

def low_keep(v):
    return (low(v), None)

def low_pass(kept, grad):
    return (grad,)

def back_keep(v):
    return (v, None)

def back_low(kept, grad):
    return (low(grad),)
low.defvjp(low_keep, low_pass)
low_back.defvjp(back_keep, back_low)
EPSILON = 1e-05
NORM_FLOOR = 1e-07
COEF_FIRST = 3.4445
COEF_SECOND = -4.775
COEF_THIRD = 2.0315
MOMENTUM = 0.9
MATRIX_RATE = 0.5
VECTOR_RATE = 0.1
MASKED = -1000000000.0
HIGHEST = lax.Precision.HIGHEST

def matmul_high(left, right):
    return jnp.dot(left, right, precision=HIGHEST)

def rotary_tables(row_count):
    half_width = ROT // 2
    frequency = jnp.power(10000.0, -jnp.arange(half_width, dtype=jnp.float32) * 2.0 / ROT)
    angles = (jnp.arange(row_count) % LEN).astype(jnp.float32)[:, None] * frequency[None, :]
    return (jnp.cos(angles)[:, None, :], jnp.sin(angles)[:, None, :])

def rotate(values, cosine, sine_table):
    half_width = ROT // 2
    first_half = values[..., :half_width]
    second_half = values[..., half_width:ROT]
    return jnp.concatenate([first_half * cosine - second_half * sine_table, second_half * cosine + first_half * sine_table, values[..., ROT:]], axis=-1)

def attend_block(queries, key_heads, values, block_start):
    score_scale = 1.0 / math.sqrt(HD)
    scores = jnp.einsum('qhd,khd->hqk', queries, key_heads, precision=HIGHEST) * score_scale
    query_place = block_start + jnp.arange(queries.shape[0])
    key_place = jnp.arange(key_heads.shape[0])
    allowed = key_place[None, :] <= query_place[:, None]
    scores = low_back(jnp.where(allowed[None], scores, MASKED))
    weights_low = low(jax.nn.softmax(scores, axis=-1))
    return jnp.einsum('hqk,khd->qhd', weights_low, values, precision=HIGHEST)

def attend_sequence(packed):
    queries, key_heads, values = packed
    outputs = []
    for block_index in range(LEN // BLOCK):
        start_row = block_index * BLOCK
        end_row = start_row + BLOCK
        block_fn = jax.checkpoint(partial(attend_block, block_start=start_row))
        outputs.append(block_fn(queries[start_row:end_row], key_heads[:end_row], values[:end_row]))
    return jnp.concatenate(outputs, 0)

def layer_forward(tokens_f, parameters):
    first_gain, first_shift, second_gain, second_shift, query_weight, key_weight, value_weight, query_bias, value_bias, output_weight, up_weight, up_bias, down_weight, out_bias = parameters
    row_count = tokens_f.shape[0]
    head_count = D // HD
    mean_value = lax.optimization_barrier(jnp.mean(tokens_f, -1, keepdims=True))
    centered = tokens_f - mean_value
    variance = lax.optimization_barrier(jnp.mean(centered * centered, -1, keepdims=True))
    normed = centered * lax.rsqrt(variance + EPSILON)
    first_input = low(normed * first_gain + first_shift)
    second_input = low(normed * second_gain + second_shift)
    cosine, sine_table = rotary_tables(row_count)
    head_shape = (row_count, head_count, HD)
    query_linear = low_back(matmul_high(first_input, low(query_weight)) + query_bias)
    key_linear = low_back(matmul_high(first_input, low(key_weight)))
    values = low(low_back(matmul_high(first_input, low(value_weight)) + value_bias))
    queries = low(rotate(query_linear.reshape(head_shape), cosine, sine_table))
    key_heads = low(rotate(key_linear.reshape(head_shape), cosine, sine_table))
    sequence_shape = (row_count // LEN, LEN, head_count, HD)
    attended = lax.map(attend_sequence, (queries.reshape(sequence_shape), key_heads.reshape(sequence_shape), values.reshape(sequence_shape)))
    attended = low(low_back(attended.reshape(row_count, D)))
    hidden = low(jax.nn.gelu(low_back(matmul_high(second_input, low(up_weight)) + up_bias), approximate=False))
    branch = matmul_high(attended, low(output_weight)) + matmul_high(hidden, low(down_weight))
    return tokens_f + branch + out_bias

def group_step(running, inputs, parameters):
    tokens_group, cotangent_group = inputs
    forward_out, pullback = jax.vjp(layer_forward, tokens_group.astype(jnp.float32), parameters)
    tokens_back, gradients = pullback(cotangent_group.astype(jnp.float32))
    running = jax.tree.map(jnp.add, running, gradients)
    return (running, (forward_out.astype(jnp.bfloat16), tokens_back))

def orthogonalize(moment):
    iterate = moment / (jnp.sqrt(jnp.sum(moment * moment)) + NORM_FLOOR)
    for step_index in range(ITERS):
        gram_matrix = matmul_high(iterate, iterate.T)
        image_term = matmul_high(gram_matrix, iterate)
        second_image = matmul_high(gram_matrix, image_term)
        iterate = COEF_FIRST * iterate + COEF_SECOND * image_term + COEF_THIRD * second_image
    return iterate

def reference(tokens, cotangent, first_gain, first_shift, second_gain, second_shift, query_weight, key_weight, value_weight, query_bias, value_bias, output_weight, up_weight, up_bias, down_weight, out_bias, first_gain_moment, first_shift_moment, second_gain_moment, second_shift_moment, query_moment, key_moment, value_moment, query_bias_moment, value_bias_moment, output_moment, up_moment, up_bias_moment, down_moment, out_bias_moment):
    parameters = (first_gain, first_shift, second_gain, second_shift, query_weight, key_weight, value_weight, query_bias, value_bias, output_weight, up_weight, up_bias, down_weight, out_bias)
    moments = (first_gain_moment, first_shift_moment, second_gain_moment, second_shift_moment, query_moment, key_moment, value_moment, query_bias_moment, value_bias_moment, output_moment, up_moment, up_bias_moment, down_moment, out_bias_moment)
    group_count = TOKENS // TOK_DEV
    start_sums = tuple((jnp.zeros_like(member) for member in parameters))
    gradients, (result, tokens_grad) = lax.scan(partial(group_step, parameters=parameters), start_sums, (tokens.reshape(group_count, TOK_DEV, D), cotangent.reshape(group_count, TOK_DEV, D)))
    result = result.reshape(TOKENS, D)
    tokens_grad = tokens_grad.reshape(TOKENS, D)
    new_moments = tuple((MOMENTUM * moment + gradient for moment, gradient in zip(moments, gradients)))
    up_scale = math.sqrt(max(1.0, FF / D))
    directions = {4: orthogonalize(new_moments[4]), 5: orthogonalize(new_moments[5]), 6: orthogonalize(new_moments[6]), 9: orthogonalize(new_moments[9].T).T, 10: up_scale * orthogonalize(new_moments[10]), 12: orthogonalize(new_moments[12].T).T}
    vector_step = VECTOR_RATE / math.sqrt(TOKENS)
    new_values = tuple((parameters[position] - MATRIX_RATE * directions[position] if position in directions else parameters[position] - vector_step * new_moments[position] for position in range(14)))
    first_gain_grad, first_shift_grad, second_gain_grad, second_shift_grad, query_weight_grad, key_weight_grad, value_weight_grad, query_bias_grad, value_bias_grad, output_weight_grad, up_weight_grad, up_bias_grad, down_weight_grad, out_bias_grad = gradients
    first_gain_moment_new, first_shift_moment_new, second_gain_moment_new, second_shift_moment_new, query_moment_new, key_moment_new, value_moment_new, query_bias_moment_new, value_bias_moment_new, output_moment_new, up_moment_new, up_bias_moment_new, down_moment_new, out_bias_moment_new = new_moments
    first_gain_new, first_shift_new, second_gain_new, second_shift_new, query_weight_new, key_weight_new, value_weight_new, query_bias_new, value_bias_new, output_weight_new, up_weight_new, up_bias_new, down_weight_new, out_bias_new = new_values
    return (result, tokens_grad, first_gain_grad, first_shift_grad, second_gain_grad, second_shift_grad, query_weight_grad, key_weight_grad, value_weight_grad, query_bias_grad, value_bias_grad, output_weight_grad, up_weight_grad, up_bias_grad, down_weight_grad, out_bias_grad, first_gain_moment_new, first_shift_moment_new, second_gain_moment_new, second_shift_moment_new, query_moment_new, key_moment_new, value_moment_new, query_bias_moment_new, value_bias_moment_new, output_moment_new, up_moment_new, up_bias_moment_new, down_moment_new, out_bias_moment_new, first_gain_new, first_shift_new, second_gain_new, second_shift_new, query_weight_new, key_weight_new, value_weight_new, query_bias_new, value_bias_new, output_weight_new, up_weight_new, up_bias_new, down_weight_new, out_bias_new)
```

```python
from functools import partial
import math

import jax
import jax.numpy as jnp
from jax import lax
from jax.experimental import pallas as pl
from jax.experimental.pallas import tpu as pltpu
from jax.sharding import PartitionSpec as P

D = 1024
HD = 64
ROT = 16
FF = 4096
LEN = 1024
ITERS = 5

EPSILON = 1e-05
NORM_FLOOR = 1e-07
COEF_FIRST = 3.4445
COEF_SECOND = -4.775
COEF_THIRD = 2.0315
MOMENTUM = 0.9
MATRIX_RATE = 0.5
VECTOR_RATE = 0.1
MASKED = -1000000000.0
PAIR = 2 * HD
ROWS_STEP = 256
MESH = pl.DeviceIdType.MESH
F32 = jnp.float32
BF16 = jnp.bfloat16

OWNERS = ((1, 1), (6, 0), (4, 1), (2, 0), (3, 0), (5, 1))


def low_product(left, right):
    return jnp.dot(left, right, preferred_element_type=F32)


def times_transpose(left, right):
    return lax.dot_general(left, right, (((1,), (1,)), ((), ())), preferred_element_type=F32)


def inner_rows(left, right):
    return lax.dot_general(left, right, (((0,), (0,)), ((), ())), preferred_element_type=F32)


def three_pass(left, right):
    return jnp.dot(left, right, precision=lax.Precision.HIGH)


def rotary_tables():
    half = ROT // 2
    lane = jnp.arange(PAIR) % HD
    frequency = jnp.power(10000.0, -(lane % half).astype(F32) * 2.0 / ROT)
    angles = jnp.arange(LEN).astype(F32)[:, None] * frequency[None, :]
    cosine, sine = jnp.cos(angles), jnp.sin(angles)
    keep = jnp.where(lane < ROT, cosine, 1.0)
    ahead = jnp.where(lane < half, -sine, 0.0)
    behind = jnp.where((lane >= half) & (lane < ROT), sine, 0.0)
    return keep, ahead, behind


def attention_kernel(
    query_ref, key_ref, value_ref, back_ref, keep_ref, ahead_ref, behind_ref,
    out_ref, query_back_ref, key_back_ref, value_back_ref,
    queries, keys, values, query_sum, key_sum, value_sum, out_sum,
):
    half = ROT // 2
    scale = 1.0 / math.sqrt(HD)
    keep, ahead, behind = keep_ref[...], ahead_ref[...], behind_ref[...]

    def rotated(x, sign):
        up = pltpu.roll(x, PAIR - half, 1)
        down = pltpu.roll(x, half, 1)
        return x * keep + sign * (up * ahead + down * behind)

    queries[...] = (rotated(query_ref[...], 1.0).astype(BF16).astype(F32) * scale).astype(BF16)
    keys[...] = rotated(key_ref[...], 1.0).astype(BF16)
    values[...] = value_ref[...].astype(BF16)
    key_sum[...] = jnp.zeros_like(key_sum)
    value_sum[...] = jnp.zeros_like(value_sum)
    query_sum[...] = jnp.zeros_like(query_sum)
    out_sum[...] = jnp.zeros_like(out_sum)
    step = ROWS_STEP
    lower = lax.broadcasted_iota(jnp.int32, (step, step), 1) <= lax.broadcasted_iota(
        jnp.int32, (step, step), 0
    )
    lanes = lax.broadcasted_iota(jnp.int32, (step, PAIR), 1) // HD

    def head(place, carry):
        mine = lanes == place
        for block in range(LEN // step):
            rows = slice(block * step, (block + 1) * step)
            width = (block + 1) * step
            query = jnp.where(mine, queries[rows, :], 0).astype(BF16)
            back = jnp.where(mine, back_ref[rows, :], 0).astype(BF16)
            scores = times_transpose(query, keys[:width, :])
            last = jnp.where(lower, scores[:, width - step :], MASKED)
            if block:
                scores = jnp.concatenate([scores[:, : width - step], last], axis=1)
            else:
                scores = last
            raised = jnp.exp(scores - jnp.max(scores, axis=1, keepdims=True))
            probs = raised * (1.0 / jnp.sum(raised, axis=1, keepdims=True))
            probs_low = probs.astype(BF16)
            probs_back = times_transpose(back, values[:width, :])
            delta = jnp.sum(probs * probs_back, axis=1, keepdims=True)
            scores_back = (probs * (probs_back - delta)).astype(BF16)
            out_sum[rows, :] += jnp.where(mine, low_product(probs_low, values[:width, :]), 0.0)
            query_sum[rows, :] += jnp.where(mine, low_product(scores_back, keys[:width, :]), 0.0)
            key_sum[:width, :] += inner_rows(scores_back, query)
            value_sum[:width, :] += inner_rows(probs_low, back)
        return carry

    lax.fori_loop(0, PAIR // HD, head, 0)
    out_ref[...] = out_sum[...].astype(BF16)
    query_back_ref[...] = rotated(query_sum[...] * scale, -1.0).astype(BF16)
    key_back_ref[...] = rotated(key_sum[...], -1.0).astype(BF16)
    value_back_ref[...] = value_sum[...].astype(BF16)


def attention(projected, attended_back, tables):
    rows, width = attended_back.shape
    pairs = width // PAIR
    piece = (LEN, PAIR)
    table = pl.BlockSpec(piece, lambda s, p: (0, 0), pipeline_mode=pl.Buffered(1))
    plain = pl.BlockSpec(piece, lambda s, p: (s, p))
    shape = jax.ShapeDtypeStruct((rows, width), BF16)
    products = 6 * rows * LEN * PAIR * pairs * 2
    return pl.pallas_call(
        attention_kernel,
        grid=(rows // LEN, pairs),
        in_specs=[
            plain,
            pl.BlockSpec(piece, lambda s, p: (s, pairs + p)),
            pl.BlockSpec(piece, lambda s, p: (s, 2 * pairs + p)),
            plain,
            table,
            table,
            table,
        ],
        out_specs=[plain] * 4,
        out_shape=[shape] * 4,
        scratch_shapes=[pltpu.VMEM(piece, BF16)] * 3 + [pltpu.VMEM(piece, F32)] * 4,
        compiler_params=pltpu.CompilerParams(vmem_limit_bytes=40 << 20),
        cost_estimate=pl.CostEstimate(
            flops=products, bytes_accessed=rows * width * 22, transcendentals=rows * LEN * pairs * 2
        ),
        name="attention",
    )(projected, projected, projected, attended_back, *tables)


def on_device(row, col, here, there):
    same = (lax.axis_index("rows") == row) & (lax.axis_index("cols") == col)
    pl.when(same)(here)
    pl.when(jnp.logical_not(same))(there)


def to_all(rows, cols, source_of, goal, send, take):
    row, col = lax.axis_index("rows"), lax.axis_index("cols")

    def one(place, carry):
        to_row, to_col = place // cols, lax.rem(place, cols)
        source = source_of(place)

        def here():
            pltpu.make_async_copy(source, goal, take).start()

        def there():
            pltpu.make_async_remote_copy(
                source, goal, send, take, device_id=(to_row, to_col), device_id_type=MESH
            ).start()

        on_device(to_row, to_col, here, there)
        return carry

    lax.fori_loop(0, rows * cols, one, 0)


def collect_kernel(
    widths, rows, cols, from_ref, vector_ref, to_ref, pieces_ref,
    send, take, cross_send, cross_take, piece_send, piece_take,
):
    row, col = lax.axis_index("rows"), lax.axis_index("cols")
    half_rows = rows // 2
    depth = from_ref.shape[0]
    half_depth = depth * half_rows
    start = 0
    for place, width in enumerate(widths):
        chip, plane = OWNERS[place]
        target = 2 * chip + row // half_rows
        source = from_ref.at[:, pl.ds(start, width)]
        goal = to_ref.at[pl.ds(row * depth, depth), pl.ds(col * width, width)]

        def here(source=source, goal=goal):
            pltpu.make_async_copy(source, goal, take).start()

        def there(source=source, goal=goal, target=target, plane=plane, place=place):
            pltpu.make_async_remote_copy(
                source, goal, send.at[place], take, device_id=(target, plane), device_id_type=MESH
            ).start()

        on_device(target, plane, here, there)
        start += width
    me = row * cols + col
    to_all(rows, cols, lambda place: vector_ref.at[place], pieces_ref.at[me], piece_send, piece_take)
    for place, width in enumerate(widths):
        chip, plane = OWNERS[place]
        core = lax.rem(row, 2)

        @pl.when((row // 2 == chip) & (col == plane))
        def _(width=width, core=core, plane=plane):
            own = to_ref.at[pl.ds(core * half_depth, half_depth), pl.ds(0, cols * width)]
            pltpu.make_async_copy(own, own, take).wait()
            swap = pltpu.make_async_remote_copy(
                own,
                own,
                cross_send,
                cross_take,
                device_id=(row + 1 - 2 * core, plane),
                device_id_type=MESH,
            )
            swap.start()
            other = to_ref.at[pl.ds((1 - core) * half_depth, half_depth), pl.ds(0, cols * width)]
            swap.wait_send()
            pltpu.make_async_copy(other, other, cross_take).wait()

    start = 0
    for place, width in enumerate(widths):
        chip, plane = OWNERS[place]
        source = from_ref.at[:, pl.ds(start, width)]

        def sent(source=source, place=place):
            pltpu.make_async_copy(source, source, send.at[place]).wait()

        on_device(2 * chip + row // half_rows, plane, lambda: None, sent)
        start += width
    pltpu.make_async_copy(pieces_ref, pieces_ref, piece_take).wait()
    others = vector_ref.at[pl.ds(0, rows * cols - 1)]
    pltpu.make_async_copy(others, others, piece_send).wait()


def collect(moments, vector, widths, rows, cols):
    depth = moments.shape[0]
    return pl.pallas_call(
        partial(collect_kernel, widths, rows, cols),
        in_specs=[pl.BlockSpec(memory_space=pl.ANY)] * 2,
        out_specs=[pl.BlockSpec(memory_space=pl.ANY)] * 2,
        out_shape=[
            jax.ShapeDtypeStruct((depth * rows, cols * max(widths)), BF16),
            jax.ShapeDtypeStruct(vector.shape, F32),
        ],
        scratch_shapes=[pltpu.SemaphoreType.DMA((6,))] + [pltpu.SemaphoreType.DMA] * 5,
        compiler_params=pltpu.CompilerParams(has_side_effects=True),
        name="collect",
    )(moments, vector)


def spread_kernel(
    widths, rows, cols, from_ref, piece_ref, to_ref, pieces_ref, send, take, piece_send, piece_take
):
    row, col = lax.axis_index("rows"), lax.axis_index("cols")
    half_rows = rows // 2
    depth = to_ref.shape[0]
    core = lax.rem(row, 2)
    start = 0
    for place, width in enumerate(widths):
        chip, plane = OWNERS[place]

        @pl.when((row // 2 == chip) & (col == plane))
        def _(width=width, start=start):
            def one(number, carry):
                near, to_col = number // cols, lax.rem(number, cols)
                to_row = core * half_rows + near
                source = from_ref.at[pl.ds(near * depth, depth), pl.ds(to_col * width, width)]
                goal = to_ref.at[:, pl.ds(start, width)]

                def here():
                    pltpu.make_async_copy(source, goal, take).start()

                def there():
                    pltpu.make_async_remote_copy(
                        source, goal, send, take, device_id=(to_row, to_col), device_id_type=MESH
                    ).start()

                on_device(to_row, to_col, here, there)
                return carry

            lax.fori_loop(0, half_rows * cols, one, 0)

        start += width
    goal = pieces_ref.at[row * cols + col]
    to_all(rows, cols, lambda place: piece_ref, goal, piece_send, piece_take)
    pltpu.make_async_copy(to_ref, to_ref, take).wait()
    for place, width in enumerate(widths):
        chip, plane = OWNERS[place]

        @pl.when((row // 2 == chip) & (col == plane))
        def _(width=width):
            def one(number, carry):
                near, to_col = number // cols, lax.rem(number, cols)
                source = from_ref.at[pl.ds(near * depth, depth), pl.ds(to_col * width, width)]

                def sent():
                    pltpu.make_async_copy(source, source, send).wait()

                on_device(core * half_rows + near, to_col, lambda: None, sent)
                return carry

            lax.fori_loop(0, half_rows * cols, one, 0)

    pltpu.make_async_copy(pieces_ref, pieces_ref, piece_take).wait()
    others = pieces_ref.at[pl.ds(0, rows * cols - 1)]
    pltpu.make_async_copy(others, others, piece_send).wait()


def spread(update, piece, widths, rows, cols):
    depth = D // rows
    return pl.pallas_call(
        partial(spread_kernel, widths, rows, cols),
        in_specs=[pl.BlockSpec(memory_space=pl.ANY)] * 2,
        out_specs=[pl.BlockSpec(memory_space=pl.ANY)] * 2,
        out_shape=[
            jax.ShapeDtypeStruct((depth, sum(widths)), BF16),
            jax.ShapeDtypeStruct((rows * cols,) + piece.shape, F32),
        ],
        scratch_shapes=[pltpu.SemaphoreType.DMA] * 4,
        compiler_params=pltpu.CompilerParams(has_side_effects=True),
        name="spread",
    )(update, piece)


def swap_kernel(part_ref, whole_ref, send, take):
    row, col = lax.axis_index("rows"), lax.axis_index("cols")
    depth = part_ref.shape[0]
    core = lax.rem(row, 2)
    mine = whole_ref.at[pl.ds(pl.multiple_of(core * depth, depth), depth), :]
    copy = pltpu.make_async_remote_copy(
        part_ref, mine, send, take, device_id=(row + 1 - 2 * core, col), device_id_type=MESH
    )
    copy.start()
    whole_ref[pl.ds(pl.multiple_of(core * depth, depth), depth), :] = part_ref[...]
    copy.wait()


def swap(part):
    depth, width = part.shape
    return pl.pallas_call(
        swap_kernel,
        in_specs=[pl.BlockSpec(memory_space=pltpu.VMEM)],
        out_specs=pl.BlockSpec(memory_space=pltpu.VMEM),
        out_shape=jax.ShapeDtypeStruct((2 * depth, width), part.dtype),
        scratch_shapes=[pltpu.SemaphoreType.DMA, pltpu.SemaphoreType.DMA],
        compiler_params=pltpu.CompilerParams(has_side_effects=True),
        name="swap",
    )(part)


def orthogonalize(moments, vector, widths, rows, cols):
    size = vector.shape[0]
    lines = -(-size // (rows * cols * 128))
    vector = jnp.pad(vector, (0, rows * cols * lines * 128 - size))
    row, col = lax.axis_index("rows"), lax.axis_index("cols")
    core = row % 2
    half = D // 2
    collected, pieces = collect(
        moments, vector.reshape(rows * cols, lines, 128), widths, rows, cols
    )
    own_width = jnp.int32(0)
    for (chip, plane), width in zip(OWNERS, widths):
        own_width = jnp.where((row // 2 == chip) & (col == plane), cols * width, own_width)
    kept = lax.broadcasted_iota(jnp.int32, collected.shape, 1) < own_width
    matrix = jnp.where(kept, collected, jnp.zeros_like(collected))
    part = times_transpose(lax.dynamic_slice_in_dim(matrix, core * half, half), matrix)
    whole = swap(part)
    place = lax.broadcasted_iota(jnp.int32, whole.shape, 0) == lax.broadcasted_iota(
        jnp.int32, whole.shape, 1
    )
    total = jnp.sum(jnp.where(place, whole, 0.0))
    shrink = 1.0 / (jnp.sqrt(total) + NORM_FLOOR)
    gram = (whole * shrink) * shrink
    part = (part * shrink) * shrink
    unit = (
        lax.broadcasted_iota(jnp.int32, part.shape, 0) + core * half
        == lax.broadcasted_iota(jnp.int32, part.shape, 1)
    ).astype(F32)
    product = None
    for step in range(ITERS):
        final = step == ITERS - 1
        if product is None:
            first = three_pass(part, gram)
            changed = COEF_FIRST * part + COEF_SECOND * first + COEF_THIRD * three_pass(first, gram)
            product = COEF_FIRST * unit + COEF_SECOND * part + COEF_THIRD * first
        elif final:
            first = three_pass(product, gram)
            product = (
                COEF_FIRST * product + COEF_SECOND * first + COEF_THIRD * three_pass(first, gram)
            )
        else:
            both = jnp.concatenate([part, product], axis=0)
            first = three_pass(both, gram)
            both = COEF_FIRST * both + COEF_SECOND * first + COEF_THIRD * three_pass(first, gram)
            changed, product = both[:half], both[half:]
        if not final:
            first = three_pass(changed, gram)
            part = (
                COEF_FIRST * changed + COEF_SECOND * first + COEF_THIRD * three_pass(first, gram)
            )
            gram = swap(part)
    high = product.astype(BF16)
    rest = (product - high.astype(F32)).astype(BF16)
    update = (low_product(high, matrix) + low_product(rest, matrix)) * shrink
    update, total = spread(update.astype(BF16), jnp.sum(pieces, 0), widths, rows, cols)
    return update, total.reshape(-1)[:size]


def split_sum(part_of, cols):
    col = lax.axis_index("cols")
    if cols == 2:
        sent = part_of(1 - col).astype(BF16)
        taken = lax.ppermute(sent, "cols", [(0, 1), (1, 0)])
        return part_of(col) + taken.astype(F32)
    parts = jnp.concatenate([part_of(place) for place in range(cols)], axis=1)
    return lax.psum_scatter(parts, "cols", scatter_dimension=1, tiled=True)


def whole_width(own, cols):
    if cols == 2:
        col, width = lax.axis_index("cols"), own.shape[1]
        taken = lax.ppermute(own, "cols", [(0, 1), (1, 0)])
        whole = jnp.zeros((own.shape[0], 2 * width), own.dtype)
        whole = lax.dynamic_update_slice(whole, own, (0, col * width))
        return lax.dynamic_update_slice(whole, taken, (0, (1 - col) * width))
    return lax.all_gather(own, "cols", axis=1, tiled=True)


def full_sum(value, cols):
    if cols == 2:
        return value + lax.ppermute(value, "cols", [(0, 1), (1, 0)])
    return lax.psum(value, "cols")


def shards(
    tokens,
    cotangent,
    first_gain,
    first_shift,
    second_gain,
    second_shift,
    query_weight,
    key_weight,
    value_weight,
    query_bias,
    value_bias,
    output_weight,
    up_weight,
    up_bias,
    down_weight,
    out_bias,
    first_gain_moment,
    first_shift_moment,
    second_gain_moment,
    second_shift_moment,
    query_moment,
    key_moment,
    value_moment,
    query_bias_moment,
    value_bias_moment,
    output_moment,
    up_moment,
    up_bias_moment,
    down_moment,
    out_bias_moment,
):
    rows = lax.axis_size("rows")
    cols = lax.axis_size("cols")
    col = lax.axis_index("cols")
    row_count, local_width = tokens.shape
    hidden_width = up_bias.shape[0]
    whole_tokens = whole_width(tokens, cols)
    forward_low = jnp.concatenate([up_weight.astype(BF16), down_weight.astype(BF16).T], axis=1)
    linear_low = jnp.concatenate(
        [
            query_weight.astype(BF16),
            key_weight.astype(BF16),
            value_weight.astype(BF16),
            output_weight.astype(BF16).T,
        ],
        axis=1,
    )
    forward_full = lax.all_gather(forward_low, "rows", axis=0, tiled=True)
    linear_full = lax.all_gather(linear_low, "rows", axis=0, tiled=True)
    whole_cotangent = whole_width(cotangent, cols)
    up_full = forward_full[:, :hidden_width]
    down_full = forward_full[:, hidden_width:]
    projection = linear_full[:, : 3 * local_width]
    output_full = linear_full[:, 3 * local_width :]
    tokens_f = whole_tokens.astype(F32)
    mean_value = jnp.mean(tokens_f, -1, keepdims=True)
    centered = tokens_f - mean_value
    inverse_scale = lax.rsqrt(jnp.mean(centered * centered, -1, keepdims=True) + EPSILON)
    normed = centered * inverse_scale
    first_input = (normed * first_gain + first_shift).astype(BF16)
    second_input = (normed * second_gain + second_shift).astype(BF16)
    up_linear = low_product(second_input, up_full) + up_bias
    activation, activation_back = jax.vjp(partial(jax.nn.gelu, approximate=False), up_linear)
    hidden = activation.astype(BF16)
    hidden_back = low_product(whole_cotangent, down_full)
    up_back = activation_back(hidden_back)[0].astype(BF16)

    def reduced(part):
        return lax.psum_scatter(part, "rows", scatter_dimension=0, tiled=True)

    down_part, up_part = inner_rows(whole_cotangent, hidden), inner_rows(second_input, up_back)
    down_part, up_part, first_input = lax.optimization_barrier((down_part, up_part, first_input))
    down_sums, up_sums = reduced(down_part), reduced(up_part)
    linear_bias = jnp.concatenate([query_bias, jnp.zeros_like(query_bias), value_bias])
    projected = low_product(first_input, projection) + linear_bias
    attended_back = low_product(whole_cotangent, output_full).astype(BF16)
    attended_low, query_back, key_back, value_back = attention(
        projected, attended_back, rotary_tables()
    )

    projected_back = jnp.concatenate([query_back, key_back, value_back], axis=1)
    other_part = jnp.concatenate(
        [inner_rows(first_input, projected_back), inner_rows(whole_cotangent, attended_low)], axis=1
    )
    other_part, attended_low, projected_back = lax.optimization_barrier(
        (other_part, attended_low, projected_back)
    )
    other_sums = reduced(other_part)

    def branch_part(place):
        output_part = lax.dynamic_slice_in_dim(output_full, place * local_width, local_width)
        down_part = lax.dynamic_slice_in_dim(down_full, place * local_width, local_width)
        return times_transpose(attended_low, output_part) + times_transpose(hidden, down_part)

    branch_share = split_sum(branch_part, cols)
    result = (tokens.astype(F32) + branch_share + out_bias).astype(BF16)
    first_back = times_transpose(projected_back, projection)
    second_back = times_transpose(up_back, up_full)
    norm_partials = jnp.stack(
        [
            jnp.sum(first_back * normed, 0),
            jnp.sum(first_back, 0),
            jnp.sum(second_back * normed, 0),
            jnp.sum(second_back, 0),
        ]
    )
    normed_part = first_back * first_gain + second_back * second_gain
    row_sums = full_sum(
        jnp.stack([jnp.sum(normed_part, 1), jnp.sum(normed_part * normed, 1)]), cols
    )
    normed_back = split_sum(
        lambda place: lax.dynamic_slice_in_dim(normed_part, place * local_width, local_width, 1),
        cols,
    )
    own_normed = (tokens.astype(F32) - mean_value) * inverse_scale
    back_mean = (row_sums[0] / D)[:, None]
    cross_mean = (row_sums[1] / D)[:, None]
    tokens_grad = (
        cotangent.astype(F32)
        + (normed_back - back_mean - own_normed * cross_mean) * inverse_scale
    )
    query_weight_grad = other_sums[:, :local_width]
    key_weight_grad = other_sums[:, local_width : 2 * local_width]
    value_weight_grad = other_sums[:, 2 * local_width : 3 * local_width]
    up_weight_grad = up_sums
    output_weight_grad = other_sums[:, 3 * local_width :].T
    down_weight_grad = down_sums.T
    bias_partials = jnp.concatenate(
        [
            jnp.sum(query_back, 0, dtype=F32),
            jnp.sum(value_back, 0, dtype=F32),
            jnp.sum(up_back, 0, dtype=F32),
            jnp.sum(cotangent, 0, dtype=F32),
        ]
    )
    slots = jnp.where(
        lax.broadcasted_iota(jnp.int32, (cols, bias_partials.shape[0]), 0) == col,
        bias_partials[None],
        0.0,
    )
    query_moment_new = MOMENTUM * query_moment + query_weight_grad
    key_moment_new = MOMENTUM * key_moment + key_weight_grad
    value_moment_new = MOMENTUM * value_moment + value_weight_grad
    up_moment_new = MOMENTUM * up_moment + up_weight_grad
    output_moment_new = MOMENTUM * output_moment + output_weight_grad
    down_moment_new = MOMENTUM * down_moment + down_weight_grad
    oriented = (
        query_moment_new,
        key_moment_new,
        value_moment_new,
        up_moment_new,
        output_moment_new.T,
        down_moment_new.T,
    )
    widths = tuple(moment.shape[1] for moment in oriented)
    bounds = [sum(widths[:position]) for position in range(7)]
    packed, totals = orthogonalize(
        jnp.concatenate([moment.astype(BF16) for moment in oriented], axis=1),
        jnp.concatenate([norm_partials.reshape(-1), slots.reshape(-1)]),
        widths,
        rows,
        cols,
    )
    packed = packed.astype(F32)
    norm_totals = totals[: 4 * D].reshape(4, D)
    bias_totals = lax.dynamic_index_in_dim(
        totals[4 * D :].reshape(slots.shape), col, 0, keepdims=False
    )
    query_bias_grad = bias_totals[:local_width]
    value_bias_grad = bias_totals[local_width : 2 * local_width]
    up_bias_grad = bias_totals[2 * local_width : 2 * local_width + hidden_width]
    out_bias_grad = bias_totals[2 * local_width + hidden_width :]
    orthogonal = [packed[:, bounds[position] : bounds[position + 1]] for position in range(6)]
    up_scale = math.sqrt(max(1.0, FF / D))
    query_weight_new = query_weight - MATRIX_RATE * orthogonal[0]
    key_weight_new = key_weight - MATRIX_RATE * orthogonal[1]
    value_weight_new = value_weight - MATRIX_RATE * orthogonal[2]
    up_weight_new = up_weight - MATRIX_RATE * (up_scale * orthogonal[3])
    output_weight_new = output_weight - MATRIX_RATE * orthogonal[4].T
    down_weight_new = down_weight - MATRIX_RATE * orthogonal[5].T
    vector_step = VECTOR_RATE / math.sqrt(row_count * rows)
    first_gain_grad = norm_totals[0]
    first_shift_grad = norm_totals[1]
    second_gain_grad = norm_totals[2]
    second_shift_grad = norm_totals[3]
    first_gain_moment_new = MOMENTUM * first_gain_moment + first_gain_grad
    first_shift_moment_new = MOMENTUM * first_shift_moment + first_shift_grad
    second_gain_moment_new = MOMENTUM * second_gain_moment + second_gain_grad
    second_shift_moment_new = MOMENTUM * second_shift_moment + second_shift_grad
    query_bias_moment_new = MOMENTUM * query_bias_moment + query_bias_grad
    value_bias_moment_new = MOMENTUM * value_bias_moment + value_bias_grad
    up_bias_moment_new = MOMENTUM * up_bias_moment + up_bias_grad
    out_bias_moment_new = MOMENTUM * out_bias_moment + out_bias_grad
    first_gain_new = first_gain - vector_step * first_gain_moment_new
    first_shift_new = first_shift - vector_step * first_shift_moment_new
    second_gain_new = second_gain - vector_step * second_gain_moment_new
    second_shift_new = second_shift - vector_step * second_shift_moment_new
    query_bias_new = query_bias - vector_step * query_bias_moment_new
    value_bias_new = value_bias - vector_step * value_bias_moment_new
    up_bias_new = up_bias - vector_step * up_bias_moment_new
    out_bias_new = out_bias - vector_step * out_bias_moment_new
    return (
        result,
        tokens_grad,
        first_gain_grad,
        first_shift_grad,
        second_gain_grad,
        second_shift_grad,
        query_weight_grad,
        key_weight_grad,
        value_weight_grad,
        query_bias_grad,
        value_bias_grad,
        output_weight_grad,
        up_weight_grad,
        up_bias_grad,
        down_weight_grad,
        out_bias_grad,
        first_gain_moment_new,
        first_shift_moment_new,
        second_gain_moment_new,
        second_shift_moment_new,
        query_moment_new,
        key_moment_new,
        value_moment_new,
        query_bias_moment_new,
        value_bias_moment_new,
        output_moment_new,
        up_moment_new,
        up_bias_moment_new,
        down_moment_new,
        out_bias_moment_new,
        first_gain_new,
        first_shift_new,
        second_gain_new,
        second_shift_new,
        query_weight_new,
        key_weight_new,
        value_weight_new,
        query_bias_new,
        value_bias_new,
        output_weight_new,
        up_weight_new,
        up_bias_new,
        down_weight_new,
        out_bias_new,
    )


def solution(mesh):
    in_specs = (
        P("rows", "cols"),
        P("rows", "cols"),
        P(),
        P(),
        P(),
        P(),
        P("rows", "cols"),
        P("rows", "cols"),
        P("rows", "cols"),
        P("cols"),
        P("cols"),
        P("cols", "rows"),
        P("rows", "cols"),
        P("cols"),
        P("cols", "rows"),
        P("cols"),
        P(),
        P(),
        P(),
        P(),
        P("rows", "cols"),
        P("rows", "cols"),
        P("rows", "cols"),
        P("cols"),
        P("cols"),
        P("cols", "rows"),
        P("rows", "cols"),
        P("cols"),
        P("cols", "rows"),
        P("cols"),
    )
    out_specs = (
        P("rows", "cols"),
        P("rows", "cols"),
        P(),
        P(),
        P(),
        P(),
        P("rows", "cols"),
        P("rows", "cols"),
        P("rows", "cols"),
        P("cols"),
        P("cols"),
        P("cols", "rows"),
        P("rows", "cols"),
        P("cols"),
        P("cols", "rows"),
        P("cols"),
        P(),
        P(),
        P(),
        P(),
        P("rows", "cols"),
        P("rows", "cols"),
        P("rows", "cols"),
        P("cols"),
        P("cols"),
        P("cols", "rows"),
        P("rows", "cols"),
        P("cols"),
        P("cols", "rows"),
        P("cols"),
        P(),
        P(),
        P(),
        P(),
        P("rows", "cols"),
        P("rows", "cols"),
        P("rows", "cols"),
        P("cols"),
        P("cols"),
        P("cols", "rows"),
        P("rows", "cols"),
        P("cols"),
        P("cols", "rows"),
        P("cols"),
    )
    return jax.shard_map(shards, mesh=mesh, in_specs=in_specs, out_specs=out_specs, check_vma=False)
```

```python
from functools import partial
import math

import jax
import jax.numpy as jnp
from jax import lax
from jax.experimental import pallas as pl
from jax.experimental.pallas import tpu as pltpu
from jax.sharding import PartitionSpec as P

D = 1024
HD = 64
ROT = 16
FF = 4096
LEN = 1024
ITERS = 5

EPSILON = 1e-05
NORM_FLOOR = 1e-07
COEF_FIRST = 3.4445
COEF_SECOND = -4.775
COEF_THIRD = 2.0315
MOMENTUM = 0.9
MATRIX_RATE = 0.5
VECTOR_RATE = 0.1
MASKED = -1000000000.0
PAIR = 2 * HD
ROWS_STEP = 256
MESH = pl.DeviceIdType.MESH
F32 = jnp.float32
BF16 = jnp.bfloat16

OWNERS = ((1, 1), (6, 0), (4, 1), (2, 0), (3, 0), (5, 1))


def low_product(left, right):
    return jnp.dot(left, right, preferred_element_type=F32)


def times_transpose(left, right):
    return lax.dot_general(left, right, (((1,), (1,)), ((), ())), preferred_element_type=F32)


def inner_rows(left, right):
    return lax.dot_general(left, right, (((0,), (0,)), ((), ())), preferred_element_type=F32)


def rotary_tables():
    half = ROT // 2
    lane = jnp.arange(PAIR) % HD
    frequency = jnp.power(10000.0, -(lane % half).astype(F32) * 2.0 / ROT)
    angles = jnp.arange(LEN).astype(F32)[:, None] * frequency[None, :]
    cosine, sine = jnp.cos(angles), jnp.sin(angles)
    keep = jnp.where(lane < ROT, cosine, 1.0)
    ahead = jnp.where(lane < half, -sine, 0.0)
    behind = jnp.where((lane >= half) & (lane < ROT), sine, 0.0)
    return keep, ahead, behind


def attention_kernel(
    query_ref, key_ref, value_ref, back_ref, keep_ref, ahead_ref, behind_ref,
    out_ref, query_back_ref, key_back_ref, value_back_ref,
    queries, keys, values, query_sum, key_sum, value_sum, out_sum,
):
    half = ROT // 2
    scale = 1.0 / math.sqrt(HD)
    keep, ahead, behind = keep_ref[...], ahead_ref[...], behind_ref[...]

    def rotated(x, sign):
        up = pltpu.roll(x, PAIR - half, 1)
        down = pltpu.roll(x, half, 1)
        return x * keep + sign * (up * ahead + down * behind)

    queries[...] = (rotated(query_ref[...], 1.0).astype(BF16).astype(F32) * scale).astype(BF16)
    keys[...] = rotated(key_ref[...], 1.0).astype(BF16)
    values[...] = value_ref[...].astype(BF16)
    key_sum[...] = jnp.zeros_like(key_sum)
    value_sum[...] = jnp.zeros_like(value_sum)
    query_sum[...] = jnp.zeros_like(query_sum)
    out_sum[...] = jnp.zeros_like(out_sum)
    step = ROWS_STEP
    lower = lax.broadcasted_iota(jnp.int32, (step, step), 1) <= lax.broadcasted_iota(
        jnp.int32, (step, step), 0
    )
    lanes = lax.broadcasted_iota(jnp.int32, (step, PAIR), 1) // HD

    def head(place, carry):
        mine = lanes == place
        for block in range(LEN // step):
            rows = slice(block * step, (block + 1) * step)
            width = (block + 1) * step
            query = jnp.where(mine, queries[rows, :], 0).astype(BF16)
            back = jnp.where(mine, back_ref[rows, :], 0).astype(BF16)
            scores = times_transpose(query, keys[:width, :])
            last = jnp.where(lower, scores[:, width - step :], MASKED)
            if block:
                scores = jnp.concatenate([scores[:, : width - step], last], axis=1)
            else:
                scores = last
            raised = jnp.exp(scores - jnp.max(scores, axis=1, keepdims=True))
            probs = raised * (1.0 / jnp.sum(raised, axis=1, keepdims=True))
            probs_low = probs.astype(BF16)
            probs_back = times_transpose(back, values[:width, :])
            delta = jnp.sum(probs * probs_back, axis=1, keepdims=True)
            scores_back = (probs * (probs_back - delta)).astype(BF16)
            out_sum[rows, :] += jnp.where(mine, low_product(probs_low, values[:width, :]), 0.0)
            query_sum[rows, :] += jnp.where(mine, low_product(scores_back, keys[:width, :]), 0.0)
            key_sum[:width, :] += inner_rows(scores_back, query)
            value_sum[:width, :] += inner_rows(probs_low, back)
        return carry

    lax.fori_loop(0, PAIR // HD, head, 0)
    out_ref[...] = out_sum[...].astype(BF16)
    query_back_ref[...] = rotated(query_sum[...] * scale, -1.0).astype(BF16)
    key_back_ref[...] = rotated(key_sum[...], -1.0).astype(BF16)
    value_back_ref[...] = value_sum[...].astype(BF16)


def attention(projected, attended_back, tables):
    rows, width = attended_back.shape
    pairs = width // PAIR
    piece = (LEN, PAIR)
    table = pl.BlockSpec(piece, lambda s, p: (0, 0), pipeline_mode=pl.Buffered(1))
    plain = pl.BlockSpec(piece, lambda s, p: (s, p))
    shape = jax.ShapeDtypeStruct((rows, width), BF16)
    products = 6 * rows * LEN * PAIR * pairs * 2
    return pl.pallas_call(
        attention_kernel,
        grid=(rows // LEN, pairs),
        in_specs=[
            plain,
            pl.BlockSpec(piece, lambda s, p: (s, pairs + p)),
            pl.BlockSpec(piece, lambda s, p: (s, 2 * pairs + p)),
            plain,
            table,
            table,
            table,
        ],
        out_specs=[plain] * 4,
        out_shape=[shape] * 4,
        scratch_shapes=[pltpu.VMEM(piece, BF16)] * 3 + [pltpu.VMEM(piece, F32)] * 4,
        compiler_params=pltpu.CompilerParams(vmem_limit_bytes=40 << 20),
        cost_estimate=pl.CostEstimate(
            flops=products, bytes_accessed=rows * width * 22, transcendentals=rows * LEN * pairs * 2
        ),
        name="attention",
    )(projected, projected, projected, attended_back, *tables)


def feed_forward_kernel(
    input_ref, cotangent_ref, up_ref, down_ref, bias_ref, hidden_ref, back_ref, sum_ref
):
    @pl.when(pl.program_id(1) == 0)
    def _():
        sum_ref[...] = jnp.zeros_like(sum_ref)

    up, down, bias = up_ref[...], down_ref[...], bias_ref[...]
    total = jnp.zeros_like(bias)
    size = 128
    for number in range(input_ref.shape[0] // size):
        place = slice(number * size, (number + 1) * size)
        linear = low_product(input_ref[place, :], up) + bias
        back = low_product(cotangent_ref[place, :], down)
        share = 0.5 * lax.erf(linear * math.sqrt(0.5)) + 0.5
        density = jnp.exp(linear * linear * -0.5) * (1.0 / math.sqrt(2.0 * math.pi))
        hidden_ref[place, :] = (linear * share).astype(BF16)
        low = (back * (share + linear * density)).astype(BF16)
        back_ref[place, :] = low
        total += jnp.sum(low.astype(F32), axis=0, keepdims=True)
    sum_ref[...] += total


def feed_forward(second_input, cotangent, up_full, down_full, up_bias):
    count, width = second_input.shape[0], up_bias.shape[0]
    high, wide = min(512, count), min(512, width)
    rows_spec = pl.BlockSpec((high, D), lambda c, r: (r, 0))
    weight_spec = pl.BlockSpec((D, wide), lambda c, r: (0, c))
    line_spec = pl.BlockSpec((1, wide), lambda c, r: (0, c))
    out_spec = pl.BlockSpec((high, wide), lambda c, r: (r, c))
    return pl.pallas_call(
        feed_forward_kernel,
        grid=(width // wide, count // high),
        in_specs=[rows_spec, rows_spec, weight_spec, weight_spec, line_spec],
        out_specs=[out_spec, out_spec, line_spec],
        out_shape=[
            jax.ShapeDtypeStruct((count, width), BF16),
            jax.ShapeDtypeStruct((count, width), BF16),
            jax.ShapeDtypeStruct((1, width), F32),
        ],
        compiler_params=pltpu.CompilerParams(vmem_limit_bytes=32 << 20),
        cost_estimate=pl.CostEstimate(
            flops=4 * count * width * D,
            bytes_accessed=4 * count * (width + D) + 4 * width * D,
            transcendentals=2 * count * width,
        ),
        name="feed_forward",
    )(second_input, cotangent, up_full, down_full, up_bias[None])


def on_device(row, col, here, there):
    same = (lax.axis_index("rows") == row) & (lax.axis_index("cols") == col)
    pl.when(same)(here)
    pl.when(jnp.logical_not(same))(there)


def to_all(rows, cols, source_of, goal, send, take):
    row, col = lax.axis_index("rows"), lax.axis_index("cols")

    def one(place, carry):
        to_row, to_col = place // cols, lax.rem(place, cols)
        source = source_of(place)

        def here():
            pltpu.make_async_copy(source, goal, take).start()

        def there():
            pltpu.make_async_remote_copy(
                source, goal, send, take, device_id=(to_row, to_col), device_id_type=MESH
            ).start()

        on_device(to_row, to_col, here, there)
        return carry

    lax.fori_loop(0, rows * cols, one, 0)


def halves(value):
    high = value.astype(BF16)
    return high, (value - high.astype(F32)).astype(BF16)


def muon_kernel(
    widths, rows, cols, from_ref, vector_ref, to_ref, totals_ref,
    matrix, grams, polys, gram_own, poly_own, turned, product, update, shrink, pieces, piece,
    send, take, cross_send, cross_take, gram_send, gram_take, poly_send, poly_take,
    spread_send, spread_take, piece_send, piece_take, total_send, total_take,
):
    row, col = lax.axis_index("rows"), lax.axis_index("cols")
    core = lax.rem(row, 2)
    half_rows = rows // 2
    depth = to_ref.shape[0]
    half = D // 2
    step = ROWS_STEP
    steps = half // step
    me = row * cols + col

    def roles(action):
        start = 0
        for place, width in enumerate(widths):
            chip, plane = OWNERS[place]
            pl.when((row // 2 == chip) & (col == plane))(partial(action, width, start))
            start += width

    start = 0
    for place, width in enumerate(widths):
        chip, plane = OWNERS[place]
        target = 2 * chip + row // half_rows
        source = from_ref.at[:, pl.ds(start, width)]
        goal = matrix.at[pl.ds(row * depth, depth), pl.ds(col * width, width)]

        def here(source=source, goal=goal):
            pltpu.make_async_copy(source, goal, take).start()

        def there(source=source, goal=goal, target=target, plane=plane, place=place):
            pltpu.make_async_remote_copy(
                source, goal, send.at[place], take, device_id=(target, plane), device_id_type=MESH
            ).start()

        on_device(target, plane, here, there)
        start += width
    to_all(rows, cols, lambda place: vector_ref.at[place], pieces.at[me], piece_send, piece_take)
    pltpu.make_async_copy(pieces, pieces, piece_take).wait()
    piece[...] = jnp.sum(pieces[...], axis=0)
    to_all(rows, cols, lambda place: piece, totals_ref.at[me], total_send, total_take)

    def own_rows(size, offset=0):
        return pl.ds(pl.multiple_of(core * half + offset, size), size)

    def other_rows(size):
        return pl.ds(pl.multiple_of((1 - core) * half, size), size)

    def cross(ref, send_sem, take_sem):
        return pltpu.make_async_remote_copy(
            ref, ref, send_sem, take_sem, device_id=(row + 1 - 2 * core, col), device_id_type=MESH
        )

    def gather_halves(width, start):
        own = matrix.at[own_rows(half), pl.ds(0, cols * width)]
        other = matrix.at[other_rows(half), pl.ds(0, cols * width)]
        pltpu.make_async_copy(own, own, take).wait()
        cross(own, cross_send, cross_take).start()
        pltpu.make_async_copy(own, own, cross_send).wait()
        pltpu.make_async_copy(other, other, cross_take).wait()

    roles(gather_halves)
    is_owner, columns = False, jnp.int32(1)
    for (chip, plane), width in zip(OWNERS, widths):
        own = (row // 2 == chip) & (col == plane)
        is_owner = is_owner | own
        columns = jnp.where(own, cols * width // D, columns)

    def over_steps(body):
        def one(number, carry):
            body(pl.ds(pl.multiple_of(number * step, step), step), number * step)
            return carry

        lax.fori_loop(0, steps, one, 0)

    def precise(left, right):
        high, rest = halves(left)
        return low_product(high, right[0]) + low_product(high, right[1]) + low_product(rest, right[0])

    def share(value, ref, offset, send_sem, take_sem):
        high, rest = halves(value)
        place = own_rows(step, offset)
        ref[0, place, :] = high
        ref[1, place, :] = rest
        cross(ref.at[:, place, :], send_sem, take_sem).start()

    def shared(ref, send_sem, take_sem):
        own, other = ref.at[:, own_rows(half), :], ref.at[:, other_rows(half), :]
        pltpu.make_async_copy(own, own, send_sem).wait()
        pltpu.make_async_copy(other, other, take_sem).wait()

    @pl.when(is_owner)
    def _():
        def squares(number, total):
            part = number // columns
            block = matrix[
                pl.ds(pl.multiple_of(part * step, step), step),
                pl.ds(pl.multiple_of(lax.rem(number, columns) * D, D), D),
            ].astype(F32)
            return total + jnp.sum(block * block, axis=0, keepdims=True)

        total = lax.fori_loop(0, columns * (D // step), squares, jnp.zeros((1, D), F32))
        total = jnp.sum(total, axis=1, keepdims=True)
        shrink[...] = jnp.broadcast_to(1.0 / (jnp.sqrt(total) + NORM_FLOOR), shrink.shape)
        factor = shrink[0:1, 0:1]

        def first_gram(place, offset):
            gram_own[place, :] = jnp.zeros((step, D), F32)

            def block(number, carry):
                across = pl.ds(pl.multiple_of(number * D, D), D)
                gram_own[place, :] += times_transpose(
                    matrix[own_rows(step, offset), across], matrix[:, across]
                )
                return carry

            lax.fori_loop(0, columns, block, 0)
            value = (gram_own[place, :] * factor) * factor
            gram_own[place, :] = value
            share(value, grams.at[0], offset, gram_send.at[0], gram_take.at[0])

        over_steps(first_gram)
        shared(grams.at[0], gram_send.at[0], gram_take.at[0])

        def iteration(number, carry):
            now = lax.rem(number, 2)
            later = 1 - now
            gram, poly = grams.at[now], polys.at[now]

            def make_poly(place, offset):
                own = gram_own[place, :]
                value = COEF_SECOND * own + COEF_THIRD * precise(own, gram)
                poly_own[place, :] = value
                share(value, poly, offset, poly_send.at[now], poly_take.at[now])

            over_steps(make_poly)

            @pl.when(number < ITERS - 1)
            def _():
                def turn(place, offset):
                    turned[place, :] = COEF_FIRST * gram_own[place, :] + precise(
                        poly_own[place, :], gram
                    )

                over_steps(turn)

            @pl.when(number == 0)
            def _():
                def begin(place, offset):
                    unit = (
                        lax.broadcasted_iota(jnp.int32, (step, D), 0) + (core * half + offset)
                        == lax.broadcasted_iota(jnp.int32, (step, D), 1)
                    )
                    product[place, :] = poly_own[place, :] + jnp.where(unit, COEF_FIRST, 0.0)

                over_steps(begin)

            shared(poly, poly_send.at[now], poly_take.at[now])

            @pl.when(number < ITERS - 1)
            def _():
                def next_gram(place, offset):
                    own = turned[place, :]
                    value = COEF_FIRST * own + precise(own, poly)
                    gram_own[place, :] = value
                    share(value, grams.at[later], offset, gram_send.at[later], gram_take.at[later])

                over_steps(next_gram)

            @pl.when(number > 0)
            def _():
                def multiply(place, offset):
                    own = product[place, :]
                    product[place, :] = COEF_FIRST * own + precise(own, poly)

                over_steps(multiply)

            @pl.when(number < ITERS - 1)
            def _():
                shared(grams.at[later], gram_send.at[later], gram_take.at[later])

            return carry

        lax.fori_loop(0, ITERS, iteration, 0)

    piece_rows = 128
    near_count = piece_rows // depth

    def finish(number, carry):
        place = pl.ds(pl.multiple_of(number * piece_rows, piece_rows), piece_rows)

        @pl.when(is_owner)
        def _():
            high, rest = halves(product[place, :] * shrink[0:1, 0:1])

            def block(across, inner):
                across = pl.ds(pl.multiple_of(across * D, D), D)
                right = matrix[:, across]
                update[place, across] = (low_product(high, right) + low_product(rest, right)).astype(
                    BF16
                )
                return inner

            lax.fori_loop(0, columns, block, 0)

        def deliver(width, start):
            def one(index, inner):
                near, to_col = number * near_count + index // cols, lax.rem(index, cols)
                to_row = core * half_rows + near
                source = update.at[pl.ds(near * depth, depth), pl.ds(to_col * width, width)]
                goal = to_ref.at[:, pl.ds(start, width)]

                def here():
                    pltpu.make_async_copy(source, goal, spread_take).start()

                def there():
                    pltpu.make_async_remote_copy(
                        source,
                        goal,
                        spread_send,
                        spread_take,
                        device_id=(to_row, to_col),
                        device_id_type=MESH,
                    ).start()

                on_device(to_row, to_col, here, there)
                return inner

            lax.fori_loop(0, near_count * cols, one, 0)

        roles(deliver)
        return carry

    lax.fori_loop(0, half // piece_rows, finish, 0)

    start = 0
    for place, width in enumerate(widths):
        chip, plane = OWNERS[place]
        source = from_ref.at[:, pl.ds(start, width)]

        def sent(source=source, place=place):
            pltpu.make_async_copy(source, source, send.at[place]).wait()

        on_device(2 * chip + row // half_rows, plane, lambda: None, sent)
        start += width
    others = vector_ref.at[pl.ds(0, rows * cols - 1)]
    pltpu.make_async_copy(others, others, piece_send).wait()
    pltpu.make_async_copy(others, others, total_send).wait()
    pltpu.make_async_copy(totals_ref, totals_ref, total_take).wait()
    pltpu.make_async_copy(to_ref, to_ref, spread_take).wait()

    def delivered(width, start):
        def one(number, carry):
            near, to_col = number // cols, lax.rem(number, cols)
            source = update.at[pl.ds(near * depth, depth), pl.ds(to_col * width, width)]

            def done():
                pltpu.make_async_copy(source, source, spread_send).wait()

            on_device(core * half_rows + near, to_col, lambda: None, done)
            return carry

        lax.fori_loop(0, half_rows * cols, one, 0)

    roles(delivered)


def orthogonalize(moments, vector, widths, rows, cols):
    size, devices = vector.shape[0], rows * cols
    lines = -(-size // (devices * 1024)) * 8
    vector = jnp.pad(vector, (0, devices * lines * 128 - size)).reshape(devices, lines, 128)
    half = D // 2
    dma = pltpu.SemaphoreType.DMA
    update, totals = pl.pallas_call(
        partial(muon_kernel, widths, rows, cols),
        in_specs=[pl.BlockSpec(memory_space=pl.ANY)] * 2,
        out_specs=[pl.BlockSpec(memory_space=pl.ANY)] * 2,
        out_shape=[
            jax.ShapeDtypeStruct(moments.shape, BF16),
            jax.ShapeDtypeStruct(vector.shape, F32),
        ],
        scratch_shapes=[
            pltpu.VMEM((D, cols * max(widths)), BF16),
            pltpu.VMEM((2, 2, D, D), BF16),
            pltpu.VMEM((2, 2, D, D), BF16),
            pltpu.VMEM((half, D), F32),
            pltpu.VMEM((half, D), F32),
            pltpu.VMEM((half, D), F32),
            pltpu.VMEM((half, D), F32),
            pltpu.VMEM((half, cols * max(widths)), BF16),
            pltpu.VMEM((8, 128), F32),
            pltpu.VMEM(vector.shape, F32),
            pltpu.VMEM((lines, 128), F32),
            dma((6,)), dma, dma, dma, dma((2,)), dma((2,)), dma((2,)), dma((2,)),
            dma, dma, dma, dma, dma, dma,
        ],
        compiler_params=pltpu.CompilerParams(
            has_side_effects=True, vmem_limit_bytes=56 << 20
        ),
        name="muon",
    )(moments, vector)
    return update, totals.reshape(-1)[:size]


def split_sum(part_of, cols):
    parts = jnp.concatenate([part_of(place) for place in range(cols)], axis=1)
    return lax.psum_scatter(parts, "cols", scatter_dimension=1, tiled=True)


def whole_width(own, cols):
    if cols == 2:
        col, width = lax.axis_index("cols"), own.shape[1]
        taken = lax.ppermute(own, "cols", [(0, 1), (1, 0)])
        whole = jnp.zeros((own.shape[0], 2 * width), own.dtype)
        whole = lax.dynamic_update_slice(whole, own, (0, col * width))
        return lax.dynamic_update_slice(whole, taken, (0, (1 - col) * width))
    return lax.all_gather(own, "cols", axis=1, tiled=True)


def full_sum(value, cols):
    if cols == 2:
        return value + lax.ppermute(value, "cols", [(0, 1), (1, 0)])
    return lax.psum(value, "cols")


def shards(
    tokens,
    cotangent,
    first_gain,
    first_shift,
    second_gain,
    second_shift,
    query_weight,
    key_weight,
    value_weight,
    query_bias,
    value_bias,
    output_weight,
    up_weight,
    up_bias,
    down_weight,
    out_bias,
    first_gain_moment,
    first_shift_moment,
    second_gain_moment,
    second_shift_moment,
    query_moment,
    key_moment,
    value_moment,
    query_bias_moment,
    value_bias_moment,
    output_moment,
    up_moment,
    up_bias_moment,
    down_moment,
    out_bias_moment,
):
    rows = lax.axis_size("rows")
    cols = lax.axis_size("cols")
    col = lax.axis_index("cols")
    row_count, local_width = tokens.shape
    hidden_width = up_bias.shape[0]
    whole_tokens = whole_width(tokens, cols)
    forward_low = jnp.concatenate([up_weight.astype(BF16), down_weight.astype(BF16).T], axis=1)
    linear_low = jnp.concatenate(
        [
            query_weight.astype(BF16),
            key_weight.astype(BF16),
            value_weight.astype(BF16),
            output_weight.astype(BF16).T,
        ],
        axis=1,
    )
    forward_full = lax.all_gather(forward_low, "rows", axis=0, tiled=True)
    linear_full = lax.all_gather(linear_low, "rows", axis=0, tiled=True)
    whole_cotangent = whole_width(cotangent, cols)
    up_full = forward_full[:, :hidden_width]
    down_full = forward_full[:, hidden_width:]
    projection = linear_full[:, : 3 * local_width]
    output_full = linear_full[:, 3 * local_width :]
    tokens_f = whole_tokens.astype(F32)
    mean_value = jnp.mean(tokens_f, -1, keepdims=True)
    centered = tokens_f - mean_value
    inverse_scale = lax.rsqrt(jnp.mean(centered * centered, -1, keepdims=True) + EPSILON)
    normed = centered * inverse_scale
    first_input = (normed * first_gain + first_shift).astype(BF16)
    second_input = (normed * second_gain + second_shift).astype(BF16)
    hidden, up_back, up_sum = feed_forward(
        second_input, whole_cotangent, up_full, down_full, up_bias
    )

    def reduced(part):
        return lax.psum_scatter(part, "rows", scatter_dimension=0, tiled=True).astype(F32)

    down_part, up_part = inner_rows(whole_cotangent, hidden), inner_rows(second_input, up_back)
    down_part, up_part, first_input, late_cotangent = lax.optimization_barrier(
        (down_part, up_part, first_input, whole_cotangent)
    )
    down_sums, up_sums = reduced(down_part.astype(BF16)), reduced(up_part.astype(BF16))
    linear_bias = jnp.concatenate([query_bias, jnp.zeros_like(query_bias), value_bias])
    projected = low_product(first_input, projection) + linear_bias
    attended_back = low_product(late_cotangent, output_full).astype(BF16)
    attended_low, query_back, key_back, value_back = attention(
        projected, attended_back, rotary_tables()
    )

    attended_low, query_back, key_back, value_back, down_sums = lax.optimization_barrier(
        (attended_low, query_back, key_back, value_back, down_sums)
    )
    projected_back = jnp.concatenate([query_back, key_back, value_back], axis=1)
    other_part = jnp.concatenate(
        [inner_rows(first_input, projected_back), inner_rows(late_cotangent, attended_low)], axis=1
    )
    other_part, attended_low, projected_back = lax.optimization_barrier(
        (other_part, attended_low, projected_back)
    )
    other_sums = reduced(other_part)

    def branch_part(place):
        output_part = lax.dynamic_slice_in_dim(output_full, place * local_width, local_width)
        down_part = lax.dynamic_slice_in_dim(down_full, place * local_width, local_width)
        return times_transpose(attended_low, output_part) + times_transpose(hidden, down_part)

    if cols == 2:
        sent = branch_part(1 - col).astype(BF16)
        sent, projected_back, up_sums = lax.optimization_barrier((sent, projected_back, up_sums))
        branch_taken = lax.ppermute(sent, "cols", [(0, 1), (1, 0)])
        branch_own = branch_part(col)
    else:
        branch_taken, branch_own = jnp.zeros((), BF16), split_sum(branch_part, cols)
    first_back = times_transpose(projected_back, projection)
    second_back = times_transpose(up_back, up_full)
    norm_partials = jnp.stack(
        [
            jnp.sum(first_back * normed, 0),
            jnp.sum(first_back, 0),
            jnp.sum(second_back * normed, 0),
            jnp.sum(second_back, 0),
        ]
    )
    normed_part = first_back * first_gain + second_back * second_gain
    row_sums = full_sum(
        jnp.stack([jnp.sum(normed_part, 1), jnp.sum(normed_part * normed, 1)]), cols
    )
    def normed_place(place):
        return lax.dynamic_slice_in_dim(normed_part, place * local_width, local_width, 1)

    if cols == 2:
        sent, branch_taken = lax.optimization_barrier(
            (normed_place(1 - col).astype(BF16), branch_taken)
        )
        taken = lax.ppermute(sent, "cols", [(0, 1), (1, 0)])
        normed_back = normed_place(col) + taken.astype(F32)
    else:
        normed_back = split_sum(normed_place, cols)
    result = (tokens.astype(F32) + branch_own + branch_taken.astype(F32) + out_bias).astype(BF16)
    own_normed = (tokens.astype(F32) - mean_value) * inverse_scale
    back_mean = (row_sums[0] / D)[:, None]
    cross_mean = (row_sums[1] / D)[:, None]
    tokens_grad = (
        cotangent.astype(F32)
        + (normed_back - back_mean - own_normed * cross_mean) * inverse_scale
    )
    query_weight_grad = other_sums[:, :local_width]
    key_weight_grad = other_sums[:, local_width : 2 * local_width]
    value_weight_grad = other_sums[:, 2 * local_width : 3 * local_width]
    up_weight_grad = up_sums
    output_weight_grad = other_sums[:, 3 * local_width :].T
    down_weight_grad = down_sums.T
    bias_partials = jnp.concatenate(
        [
            jnp.sum(query_back, 0, dtype=F32),
            jnp.sum(value_back, 0, dtype=F32),
            up_sum[0],
            jnp.sum(cotangent, 0, dtype=F32),
        ]
    )
    slots = jnp.where(
        lax.broadcasted_iota(jnp.int32, (cols, bias_partials.shape[0]), 0) == col,
        bias_partials[None],
        0.0,
    )
    query_moment_new = MOMENTUM * query_moment + query_weight_grad
    key_moment_new = MOMENTUM * key_moment + key_weight_grad
    value_moment_new = MOMENTUM * value_moment + value_weight_grad
    up_moment_new = MOMENTUM * up_moment + up_weight_grad
    output_moment_new = MOMENTUM * output_moment + output_weight_grad
    down_moment_new = MOMENTUM * down_moment + down_weight_grad
    oriented = (
        query_moment_new,
        key_moment_new,
        value_moment_new,
        up_moment_new,
        output_moment_new.T,
        down_moment_new.T,
    )
    widths = tuple(moment.shape[1] for moment in oriented)
    bounds = [sum(widths[:position]) for position in range(7)]
    packed, totals = orthogonalize(
        jnp.concatenate([moment.astype(BF16) for moment in oriented], axis=1),
        jnp.concatenate([norm_partials.reshape(-1), slots.reshape(-1)]),
        widths,
        rows,
        cols,
    )
    packed = packed.astype(F32)
    norm_totals = totals[: 4 * D].reshape(4, D)
    bias_totals = lax.dynamic_index_in_dim(
        totals[4 * D :].reshape(slots.shape), col, 0, keepdims=False
    )
    query_bias_grad = bias_totals[:local_width]
    value_bias_grad = bias_totals[local_width : 2 * local_width]
    up_bias_grad = bias_totals[2 * local_width : 2 * local_width + hidden_width]
    out_bias_grad = bias_totals[2 * local_width + hidden_width :]
    orthogonal = [packed[:, bounds[position] : bounds[position + 1]] for position in range(6)]
    up_scale = math.sqrt(max(1.0, FF / D))
    query_weight_new = query_weight - MATRIX_RATE * orthogonal[0]
    key_weight_new = key_weight - MATRIX_RATE * orthogonal[1]
    value_weight_new = value_weight - MATRIX_RATE * orthogonal[2]
    up_weight_new = up_weight - MATRIX_RATE * (up_scale * orthogonal[3])
    output_weight_new = output_weight - MATRIX_RATE * orthogonal[4].T
    down_weight_new = down_weight - MATRIX_RATE * orthogonal[5].T
    vector_step = VECTOR_RATE / math.sqrt(row_count * rows)
    first_gain_grad = norm_totals[0]
    first_shift_grad = norm_totals[1]
    second_gain_grad = norm_totals[2]
    second_shift_grad = norm_totals[3]
    first_gain_moment_new = MOMENTUM * first_gain_moment + first_gain_grad
    first_shift_moment_new = MOMENTUM * first_shift_moment + first_shift_grad
    second_gain_moment_new = MOMENTUM * second_gain_moment + second_gain_grad
    second_shift_moment_new = MOMENTUM * second_shift_moment + second_shift_grad
    query_bias_moment_new = MOMENTUM * query_bias_moment + query_bias_grad
    value_bias_moment_new = MOMENTUM * value_bias_moment + value_bias_grad
    up_bias_moment_new = MOMENTUM * up_bias_moment + up_bias_grad
    out_bias_moment_new = MOMENTUM * out_bias_moment + out_bias_grad
    first_gain_new = first_gain - vector_step * first_gain_moment_new
    first_shift_new = first_shift - vector_step * first_shift_moment_new
    second_gain_new = second_gain - vector_step * second_gain_moment_new
    second_shift_new = second_shift - vector_step * second_shift_moment_new
    query_bias_new = query_bias - vector_step * query_bias_moment_new
    value_bias_new = value_bias - vector_step * value_bias_moment_new
    up_bias_new = up_bias - vector_step * up_bias_moment_new
    out_bias_new = out_bias - vector_step * out_bias_moment_new
    return (
        result,
        tokens_grad,
        first_gain_grad,
        first_shift_grad,
        second_gain_grad,
        second_shift_grad,
        query_weight_grad,
        key_weight_grad,
        value_weight_grad,
        query_bias_grad,
        value_bias_grad,
        output_weight_grad,
        up_weight_grad,
        up_bias_grad,
        down_weight_grad,
        out_bias_grad,
        first_gain_moment_new,
        first_shift_moment_new,
        second_gain_moment_new,
        second_shift_moment_new,
        query_moment_new,
        key_moment_new,
        value_moment_new,
        query_bias_moment_new,
        value_bias_moment_new,
        output_moment_new,
        up_moment_new,
        up_bias_moment_new,
        down_moment_new,
        out_bias_moment_new,
        first_gain_new,
        first_shift_new,
        second_gain_new,
        second_shift_new,
        query_weight_new,
        key_weight_new,
        value_weight_new,
        query_bias_new,
        value_bias_new,
        output_weight_new,
        up_weight_new,
        up_bias_new,
        down_weight_new,
        out_bias_new,
    )


def solution(mesh):
    in_specs = (
        P("rows", "cols"),
        P("rows", "cols"),
        P(),
        P(),
        P(),
        P(),
        P("rows", "cols"),
        P("rows", "cols"),
        P("rows", "cols"),
        P("cols"),
        P("cols"),
        P("cols", "rows"),
        P("rows", "cols"),
        P("cols"),
        P("cols", "rows"),
        P("cols"),
        P(),
        P(),
        P(),
        P(),
        P("rows", "cols"),
        P("rows", "cols"),
        P("rows", "cols"),
        P("cols"),
        P("cols"),
        P("cols", "rows"),
        P("rows", "cols"),
        P("cols"),
        P("cols", "rows"),
        P("cols"),
    )
    out_specs = (
        P("rows", "cols"),
        P("rows", "cols"),
        P(),
        P(),
        P(),
        P(),
        P("rows", "cols"),
        P("rows", "cols"),
        P("rows", "cols"),
        P("cols"),
        P("cols"),
        P("cols", "rows"),
        P("rows", "cols"),
        P("cols"),
        P("cols", "rows"),
        P("cols"),
        P(),
        P(),
        P(),
        P(),
        P("rows", "cols"),
        P("rows", "cols"),
        P("rows", "cols"),
        P("cols"),
        P("cols"),
        P("cols", "rows"),
        P("rows", "cols"),
        P("cols"),
        P("cols", "rows"),
        P("cols"),
        P(),
        P(),
        P(),
        P(),
        P("rows", "cols"),
        P("rows", "cols"),
        P("rows", "cols"),
        P("cols"),
        P("cols"),
        P("cols", "rows"),
        P("rows", "cols"),
        P("cols"),
        P("cols", "rows"),
        P("cols"),
    )
    return jax.shard_map(shards, mesh=mesh, in_specs=in_specs, out_specs=out_specs, check_vma=False)
```
